32 devices in a mesh: fine: 8 (over z, core), sub: 2 (over x), dp: 2 (over y).
Axes of the slice: x: 2, y: 2, z: 4, core: 2. Of those that a mesh axis runs over, the one named last changes fastest.
Arguments:
- queries: bfloat16 [2, 1024, 512], P('dp', 'fine', 'sub'), may hold values from -6 to 6
- keys: bfloat16 [2, 1024, 512], P('dp', 'fine', 'sub'), may hold values from -6 to 6
- values: bfloat16 [2, 1024, 512], P('dp', 'fine', 'sub'), may hold values from -6 to 6
- out_grad: bfloat16 [2, 1024, 512], P('dp', 'fine', 'sub'), may hold values from -6 to 6
- coarse_keys: bfloat16 [2, 512, 512], P(None, ('fine', 'sub', 'dp')), may hold values from -6 to 6
- coarse_values: bfloat16 [2, 512, 512], P(None, ('fine', 'sub', 'dp')), may hold values from -6 to 6
- fine_scale: int32 [1024], replicated, may hold values from 0 to 2, never falling along the last dimension, each value on 1 to 640 neighbouring positions
Outputs:
- attended: bfloat16 [2, 1024, 512], P('dp', 'fine', 'sub')
- query_grad: bfloat16 [2, 1024, 512], P('dp', 'fine', 'sub')
- key_grad: bfloat16 [2, 1024, 512], P('dp', 'fine', 'sub')
- value_grad: bfloat16 [2, 1024, 512], P('dp', 'fine', 'sub')
- coarse_key_grad: bfloat16 [2, 512, 512], P(None, ('fine', 'sub', 'dp'))
- coarse_value_grad: bfloat16 [2, 512, 512], P(None, ('fine', 'sub', 'dp'))
The draws below stay inside these ranges and needn't reach their ends.
Inputs may be any that keep to these rules, and one draw needn't show every extreme that they name: `fine_scale`: the scale of each fine token among the last three scales, numbered from 0; it never falls along the tokens and every scale holds at least one token.
All inputs are finite; a program needn't handle non-finite values.
Results may differ from the reference program's by a relative error of at most 0.0098.
Values may be sent and summed in bfloat16 or wider, within the bound.
A program may use at most 64 MiB of HBM per device.

```python
import math
import jax
import jax.numpy as jnp
import numpy as np
from jax import lax

HEAD = 128
COARSE = 512
WIDTH = 512
FINE = 1024
IMAGES = 2


def draw_queries(key, part):
    entries = jax.random.normal(jax.random.fold_in(key, 21), (IMAGES, FINE, WIDTH), jnp.float32)
    entries = jnp.clip(entries, -6.0, 6.0)
    return entries.astype(jnp.bfloat16)


def draw_coarse_keys(key, part):
    entries = jax.random.normal(jax.random.fold_in(key, 31), (IMAGES, COARSE, WIDTH), jnp.float32)
    entries = jnp.clip(entries, -6.0, 6.0)
    return entries.astype(jnp.bfloat16)


def steps_of(own_key, dims, shards, least, high):
    level = 1.0
    for axis_at, shards_of in shards:
        heights = jax.random.uniform(jax.random.fold_in(jax.random.fold_in(own_key, 6), axis_at), (shards_of,), jnp.float32, least / len(shards), high / len(shards))
        level = level * jnp.repeat(jnp.exp(heights), dims[axis_at] // shards_of).reshape((-1,) + (1,) * (len(dims) - 1 - axis_at))
    return level


def length_profile(number_of, total, reach, slope):
    weights = [(1 << 20) // math.isqrt(standing ** slope) + 1 for standing in range(2, number_of + 1)]
    surplus, given = total - reach - (number_of - 1), [1] * (number_of - 1)
    while surplus > 0:
        free = [i for i in range(number_of - 1) if given[i] < reach]
        pool, remaining = sum([weights[i] for i in free]), surplus
        for i in free:
            more = min(reach - given[i], max(1, remaining * weights[i] // pool), surplus)
            given[i] = given[i] + more
            surplus = surplus - more
    return np.array([reach] + given)


def uneven_parts(stream_key, number_of, total, most, slope):
    if number_of == 2:
        one = jax.random.randint(stream_key, (), max(1, total - most), min(most, total - 1) + 1)
        return jnp.stack([one, total - one])
    tallies = jnp.asarray(length_profile(number_of, total, most, slope), jnp.int32)
    twos = (number_of - 1) // 2
    donor, sink = tallies[1:1 + 2 * twos:2], tallies[2:2 + 2 * twos:2]
    margin = jnp.minimum(donor - 1, most - sink)
    moved = jax.random.randint(jax.random.fold_in(stream_key, 1), (twos,), 0, 1 << 20) % (margin + 1)
    tallies = tallies.at[1:1 + 2 * twos:2].set(donor - moved).at[2:2 + 2 * twos:2].set(sink + moved)
    return tallies[jax.random.permutation(jax.random.fold_in(stream_key, 2), number_of)]


def gaussian(stream_key, extent, width, most, cuts=(), kind=jnp.bfloat16):
    values = jax.random.normal(stream_key, extent, jnp.float32) * width
    if len(cuts) > 0:
        values = steps_of(stream_key, extent, cuts, -0.22, 0.18) * values
    return jnp.clip(values, min=-most, max=most).astype(kind)


def setup_inputs(seed: int = 0) -> dict:
    seeds = jax.random.split(jax.random.key(seed), 8)
    queries = draw_queries(jax.random.fold_in(seeds[7], 71), 0)
    keys = gaussian(seeds[1], (IMAGES, FINE, WIDTH), 1.0, 6.0, ((0, 2), (1, 8), (2, 2)))
    values = gaussian(seeds[2], (IMAGES, FINE, WIDTH), 1.0, 6.0, ((0, 2), (1, 8), (2, 2)))
    out_grad = gaussian(seeds[3], (IMAGES, FINE, WIDTH), 1.0, 6.0, ((0, 2), (1, 8), (2, 2)))
    coarse_keys = draw_coarse_keys(jax.random.fold_in(seeds[7], 71), 0)
    coarse_values = gaussian(seeds[5], (IMAGES, COARSE, WIDTH), 1.0, 6.0, ((1, 32),))
    fine_scale = jnp.searchsorted(jnp.cumsum(uneven_parts(seeds[6], 3, FINE, FINE * 5 // 8, 0)), jnp.arange(FINE), side="right").astype(jnp.int32)
    return {"queries": queries, "keys": keys, "values": values, "out_grad": out_grad, "coarse_keys": coarse_keys, "coarse_values": coarse_values, "fine_scale": fine_scale}


def attend_block(query_block, grad_block, keys_head, values_head, query_scale, key_scale):
    inverse = 1.0 / math.sqrt(HEAD)
    scores = jnp.dot(query_block, keys_head.T, preferred_element_type=jnp.float32) * inverse
    visible = key_scale[None, :] <= query_scale[:, None]
    row_peak = lax.optimization_barrier(jnp.max(jnp.where(visible, scores, -jnp.inf), axis=1))
    row_total = lax.optimization_barrier(jnp.sum(jnp.exp(jnp.where(visible, scores - row_peak[:, None], -jnp.inf)), axis=1))
    log_total = row_peak + jnp.log(row_total)
    weights = jnp.exp(jnp.where(visible, scores - log_total[:, None], -jnp.inf)).astype(jnp.bfloat16)
    weights = lax.optimization_barrier(weights)
    attended = jnp.dot(weights, values_head, preferred_element_type=jnp.float32).astype(jnp.bfloat16)
    attended = lax.optimization_barrier(attended)
    row_delta = lax.optimization_barrier(jnp.sum(grad_block.astype(jnp.float32) * attended.astype(jnp.float32), axis=1))
    value_dots = jnp.dot(grad_block, values_head.T, preferred_element_type=jnp.float32)
    score_grads = (weights.astype(jnp.float32) * (value_dots - row_delta[:, None]) * inverse).astype(jnp.bfloat16)
    query_grad = jnp.dot(score_grads, keys_head, preferred_element_type=jnp.float32).astype(jnp.bfloat16)
    key_part = jnp.dot(score_grads.T, query_block, preferred_element_type=jnp.float32)
    value_part = jnp.dot(weights.T, grad_block, preferred_element_type=jnp.float32)
    return (attended, query_grad, key_part, value_part)

def single_image(queries, keys, values, out_grad, coarse_keys, coarse_values, fine_scale):
    head_count = queries.shape[1] // HEAD
    block_rows = min(FINE, 2048)
    blocks = FINE // block_rows
    scale_ids = fine_scale.astype(jnp.int32)
    key_scale = jnp.concatenate([jnp.full((COARSE,), -1, jnp.int32), scale_ids])

    def by_head(matrix):
        return matrix.reshape(matrix.shape[0], head_count, HEAD).transpose(1, 0, 2)
    all_keys = by_head(jnp.concatenate([coarse_keys, keys], axis=0))
    all_values = by_head(jnp.concatenate([coarse_values, values], axis=0))

    def one_head(operands):
        query_head, grad_head, keys_head, values_head = operands

        def block_step(running, position):
            first_row = position * block_rows
            query_block = lax.dynamic_slice_in_dim(query_head, first_row, block_rows, 0)
            grad_block = lax.dynamic_slice_in_dim(grad_head, first_row, block_rows, 0)
            query_scale = lax.dynamic_slice_in_dim(scale_ids, first_row, block_rows, 0)
            attended, query_grad, key_part, value_part = attend_block(query_block, grad_block, keys_head, values_head, query_scale, key_scale)
            return ((running[0] + key_part, running[1] + value_part), (attended, query_grad))
        zero_grads = jnp.zeros((COARSE + FINE, HEAD), jnp.float32)
        totals, produced = lax.scan(block_step, (zero_grads, zero_grads), jnp.arange(blocks, dtype=jnp.int32))
        return (produced[0].reshape(FINE, HEAD), produced[1].reshape(FINE, HEAD), totals[0], totals[1])
    outputs = lax.map(one_head, (by_head(queries), by_head(out_grad), all_keys, all_values))

    def merged(stacked):
        return stacked.transpose(1, 0, 2).reshape(stacked.shape[1], head_count * HEAD)
    attended = merged(outputs[0])
    query_grad = merged(outputs[1])
    key_total = merged(outputs[2])
    value_total = merged(outputs[3])
    return (attended, query_grad, key_total[COARSE:].astype(jnp.bfloat16), value_total[COARSE:].astype(jnp.bfloat16), key_total[:COARSE].astype(jnp.bfloat16), value_total[:COARSE].astype(jnp.bfloat16))

def reference(queries, keys, values, out_grad, coarse_keys, coarse_values, fine_scale):

    def per_image(operands):
        return single_image(operands[0], operands[1], operands[2], operands[3], operands[4], operands[5], fine_scale)
    return lax.map(per_image, (queries, keys, values, out_grad, coarse_keys, coarse_values))
```

```python
import functools
import math

import jax
import jax.numpy as jnp
from jax import lax
from jax.experimental import pallas as pl
from jax.experimental.pallas import tpu as pltpu
from jax.sharding import PartitionSpec as P

HEAD = 128
CORES = 2
MESH = pl.DeviceIdType.MESH
INVERSE = 1.0 / math.sqrt(HEAD)


def nt(a, b):
    return lax.dot_general(a, b, (((1,), (1,)), ((), ())), preferred_element_type=jnp.float32)


def tn(a, b):
    return lax.dot_general(a, b, (((0,), (0,)), ((), ())), preferred_element_type=jnp.float32)


def nn(a, b):
    return jnp.dot(a, b, preferred_element_type=jnp.float32)


def wait_bytes(ref, sem):
    pltpu.make_async_copy(ref, ref, sem).wait()


def kernel(
    sizes,
    direct,
    queries,
    keys,
    values,
    out_grad,
    coarse_keys,
    coarse_values,
    scale_in,
    attended,
    query_grad,
    key_grad,
    value_grad,
    coarse_key_grad,
    coarse_value_grad,
    scale_row,
    kv_src,
    qg_src,
    c_src,
    kv,
    qg,
    ckv,
    stats,
    stage,
    coarse_stage,
    key_acc,
    value_acc,
    load_sem,
    kv_recv,
    c_recv,
    qg_recv,
    stat_recv,
    out_recv,
    cg_recv,
    kv_send,
    c_send,
    qg_send,
    near_send,
    stat_send,
    out_send,
    cg_send,
):
    n_fine, n_sub, n_dp = sizes
    fine, sub, dp = lax.axis_index("fine"), lax.axis_index("sub"), lax.axis_index("dp")
    chip, core = fine // CORES, lax.rem(fine, CORES)
    chips = n_fine // CORES
    rows = keys.shape[1]
    span = rows * CORES
    coarse_rows = ckv.shape[1]
    coarse_span = coarse_rows // chips
    partner = {"fine": chip * CORES + (1 - core)}

    loads = []
    for slot, (src, dst) in enumerate(
        (
            (keys.at[0], kv_src.at[0]),
            (values.at[0], kv_src.at[1]),
            (coarse_keys, c_src.at[0]),
            (coarse_values, c_src.at[1]),
            (queries.at[0], qg_src.at[0]),
            (out_grad.at[0], qg_src.at[1]),
            (scale_in, scale_row),
        )
    ):
        copy = pltpu.make_async_copy(src, dst, load_sem.at[slot])
        copy.start()
        loads.append(copy)

    barrier = pltpu.get_barrier_semaphore()
    plane = []
    for step_core in range(CORES):
        for step_sub in range(n_sub if direct else 1):
            for step_dp in range(n_dp if direct else 1):
                if step_core or step_sub or step_dp:
                    plane.append(
                        (
                            chip * CORES + lax.rem(core + step_core, CORES),
                            lax.rem(sub + step_sub, n_sub),
                            lax.rem(dp + step_dp, n_dp),
                        )
                    )
    column = []
    for step_chip in range(1, chips):
        for step_core in range(CORES):
            to_chip = lax.rem(chip + step_chip, chips)
            column.append((to_chip * CORES + lax.rem(core + step_core, CORES), sub, dp))
    for other in column + plane:
        pl.semaphore_signal(barrier, inc=1, device_id=other, device_id_type=MESH)
    pl.semaphore_wait(barrier, len(column + plane))

    def head_columns(index):
        return pl.ds(pl.multiple_of(index * HEAD, HEAD), HEAD)

    my_rows = pl.ds(pl.multiple_of(fine * rows, rows), rows)
    chip_rows = pl.ds(pl.multiple_of(chip * span, span), span)
    chip_coarse = pl.ds(pl.multiple_of(chip * coarse_span, coarse_span), coarse_span)

    def remote(src, dst, send, recv, device):
        pltpu.make_async_remote_copy(
            src_ref=src,
            dst_ref=dst,
            send_sem=send,
            recv_sem=recv,
            device_id=device,
            device_id_type=MESH,
        ).start()

    def towards(right, act):
        to = chip + 1 if right else chip - 1
        pl.when(to < chips if right else to >= 0)(lambda: act(to))

    def send_own(src, dst, send, recv, right):
        def both_cores(to):
            for to_core in range(CORES):
                remote(
                    src.at[:, :, to_core * HEAD : (to_core + 1) * HEAD],
                    dst.at[:, my_rows],
                    send.at[right, 0],
                    recv.at[chip],
                    {"fine": to * CORES + to_core},
                )

        towards(right, both_cores)

    def share(src, dst, near, recv):
        remote(
            src.at[:, :, head_columns(1 - core)], dst.at[:, my_rows], near, recv.at[chip], partner
        )
        pltpu.make_async_copy(
            src.at[:, :, head_columns(core)], dst.at[:, my_rows], recv.at[chip]
        ).start()

    def block_of(at, size):
        return pl.ds(pl.multiple_of(at * size, size), size)

    def pass_on(buffer, size, send, recv, hop, right):
        at = chip - hop if right else chip + hop

        def arrived(to):
            block = buffer.at[:, block_of(at, size)]
            wait_bytes(block, recv.at[at])
            remote(block, block, send.at[right, hop], recv.at[at], {"fine": to * CORES + core})

        pl.when(at >= 0 if right else at < chips)(lambda: towards(right, arrived))

    loads[0].wait()
    loads[1].wait()
    for right in (0, 1):
        send_own(kv_src, kv, kv_send, kv_recv, right)
    share(kv_src, kv, near_send.at[0], kv_recv)
    loads[2].wait()
    loads[3].wait()
    mine = coarse_keys.shape[1]
    if direct:
        block = (fine * n_sub + sub) * n_dp + dp
    else:
        block = fine
    mine_rows = pl.ds(pl.multiple_of(block * mine, mine), mine)

    def coarse_piece(image, index):
        return c_src.at[:, image, :, head_columns(index)]

    for to_fine, to_sub, to_dp in plane:
        to_core = lax.rem(to_fine, CORES)
        piece = coarse_piece(to_dp, to_sub * CORES + to_core) if direct else coarse_piece(0, to_core)
        remote(piece, ckv.at[:, mine_rows], near_send.at[2], c_recv.at[chip], (to_fine, to_sub, to_dp))
    piece = coarse_piece(dp, sub * CORES + core) if direct else coarse_piece(0, core)
    pltpu.make_async_copy(piece, ckv.at[:, mine_rows], c_recv.at[chip]).start()
    loads[4].wait()
    loads[5].wait()
    share(qg_src, qg, near_send.at[1], qg_recv)

    own_coarse = ckv.at[:, chip_coarse]
    wait_bytes(own_coarse, c_recv.at[chip])
    for right in (0, 1):
        towards(
            right,
            lambda to, right=right: remote(
                own_coarse,
                own_coarse,
                c_send.at[right, 0],
                c_recv.at[chip],
                {"fine": to * CORES + core},
            ),
        )
    at_end = jnp.logical_or(chip == 0, chip == chips - 1)
    for hop in range(1, chips):
        for right in (0, 1):
            pass_on(kv, span, kv_send, kv_recv, hop, right)
            pass_on(ckv, coarse_span, c_send, c_recv, hop, right)
            spent = chip == hop - 1 if right else chip == chips - hop
            pl.when(spent)(
                lambda right=right: send_own(qg_src, qg, qg_send, qg_recv, right)
            )
    if chips > 2:
        for right in (0, 1):
            pass_on(qg, span, qg_send, qg_recv, 1, right)
    for step in range(1, chips):
        at = lax.rem(chip + step, chips)

        def last_stop(at=at):
            wait_bytes(kv.at[:, block_of(at, span)], kv_recv.at[at])
            wait_bytes(ckv.at[:, block_of(at, coarse_span)], c_recv.at[at])

        pl.when(at_end)(last_stop)

    loads[6].wait()
    scales = scale_row[...].astype(jnp.float32)
    own_scale = scale_row[:, chip_rows].astype(jnp.float32)
    own_column = jnp.transpose(jnp.broadcast_to(own_scale, (HEAD, span)))[:, :1]

    wait_bytes(qg.at[:, chip_rows], qg_recv.at[chip])
    query_own, grad_own = qg[0, chip_rows], qg[1, chip_rows]
    wait_bytes(kv.at[:, chip_rows], kv_recv.at[chip])
    fine_scores = nt(query_own, kv[0]) * INVERSE
    fine_scores = jnp.where(scales <= own_column, fine_scores, -jnp.inf)
    coarse_scores = nt(query_own, ckv[0]) * INVERSE
    peak = jnp.maximum(
        jnp.max(fine_scores, axis=1, keepdims=True), jnp.max(coarse_scores, axis=1, keepdims=True)
    )
    total = jnp.sum(jnp.exp(fine_scores - peak), axis=1, keepdims=True) + jnp.sum(
        jnp.exp(coarse_scores - peak), axis=1, keepdims=True
    )
    log_total = peak + jnp.log(total)
    fine_weights = jnp.exp(fine_scores - log_total).astype(jnp.bfloat16)
    coarse_weights = jnp.exp(coarse_scores - log_total).astype(jnp.bfloat16)
    for hop in range(2, chips - 1):
        for right in (0, 1):
            pass_on(qg, span, qg_send, qg_recv, hop, right)
    out = (nn(fine_weights, kv[1]) + nn(coarse_weights, ckv[1])).astype(jnp.bfloat16)
    delta = jnp.sum(
        grad_own.astype(jnp.float32) * out.astype(jnp.float32), axis=1, keepdims=True
    )
    log_rows = jnp.transpose(jnp.broadcast_to(log_total, (span, HEAD)))[:8]
    delta_rows = jnp.transpose(jnp.broadcast_to(delta, (span, HEAD)))[:8]
    first = lax.broadcasted_iota(jnp.int32, (8, span), 0) == 0
    stats[chip] = jnp.where(first, log_rows, delta_rows)
    for step in range(1, chips):
        to = lax.rem(chip + step, chips)
        remote(
            stats.at[chip],
            stats.at[chip],
            stat_send,
            stat_recv.at[chip],
            {"fine": to * CORES + core},
        )

    def hand_out(slot, value, result):
        height = value.shape[0] // CORES
        stage[slot, : value.shape[0]] = value
        give = pl.ds(pl.multiple_of((1 - core) * height, height), height)
        keep = pl.ds(pl.multiple_of(core * height, height), height)
        remote(
            stage.at[slot, give],
            result.at[0, :, head_columns(core)],
            out_send.at[slot],
            out_recv.at[slot],
            partner,
        )
        result[0, :, head_columns(core)] = stage[slot, keep]

    def collect(slot, result):
        half = result.at[0, :, head_columns(1 - core)]
        wait_bytes(half, out_recv.at[slot])
        wait_bytes(half, out_send.at[slot])

    hand_out(0, out, attended)

    def grads_of(weights, dots, row_delta):
        return (weights.astype(jnp.float32) * (dots - row_delta) * INVERSE).astype(jnp.bfloat16)

    fine_grads = grads_of(fine_weights, nt(grad_own, kv[1]), delta)
    coarse_grads = grads_of(coarse_weights, nt(grad_own, ckv[1]), delta)
    query_out = nn(fine_grads, kv[0]) + nn(coarse_grads, ckv[0])
    hand_out(1, query_out.astype(jnp.bfloat16), query_grad)

    reach = jnp.minimum(chip, chips - 1 - chip)
    longer = jnp.where(chip > chips - 1 - chip, -1, 1)
    for step in range(chips):
        near = -(step + 1) // 2 if step % 2 else step // 2
        at = chip + jnp.where(step <= 2 * reach, near, longer * (step - reach))
        at_rows = pl.ds(pl.multiple_of(at * span, span), span)
        if step:

            def last_queries(at=at, at_rows=at_rows):
                wait_bytes(qg.at[:, at_rows], qg_recv.at[at])

            pl.when(at_end)(last_queries)
            wait_bytes(stats.at[at], stat_recv.at[at])
        query_block, grad_block = qg[0, at_rows], qg[1, at_rows]
        log_row, delta_row = stats[at, 0:1], stats[at, 1:2]
        block_scale = scale_row[:, at_rows].astype(jnp.float32)
        for part in range(2):
            source, own, low = ((kv, chip_rows, 0), (ckv, chip_coarse, span))[part]
            high = low + (span, coarse_span)[part]
            scores = nt(source[0, own], query_block) * INVERSE
            if part == 0:
                scores = jnp.where(own_column <= block_scale, scores, -jnp.inf)
            weights = jnp.exp(scores - log_row).astype(jnp.bfloat16)
            value_part = nn(weights, grad_block)
            grads = grads_of(weights, nt(source[1, own], grad_block), delta_row)
            key_part = nn(grads, query_block)
            if step:
                value_part += value_acc[low:high]
                key_part += key_acc[low:high]
            value_acc[low:high] = value_part
            key_acc[low:high] = key_part

    coarse_out = (coarse_key_grad, coarse_value_grad)
    for slot, acc in enumerate((key_acc, value_acc)):
        part = acc[span:].astype(jnp.bfloat16)
        if not direct:
            hand_out(4 + slot, part, coarse_out[slot])
            continue
        coarse_stage[slot] = part
        for step_core in range(CORES):
            for step_sub in range(n_sub):
                for step_dp in range(n_dp):
                    to_core = lax.rem(core + step_core, CORES)
                    to_sub = lax.rem(sub + step_sub, n_sub)
                    to_dp = lax.rem(dp + step_dp, n_dp)
                    piece = (to_core * n_sub + to_sub) * n_dp + to_dp
                    src = coarse_stage.at[slot, pl.ds(pl.multiple_of(piece * mine, mine), mine)]
                    dst = coarse_out[slot].at[dp, :, head_columns(sub * CORES + core)]
                    if step_core or step_sub or step_dp:
                        remote(
                            src,
                            dst,
                            cg_send.at[slot],
                            cg_recv.at[slot],
                            (chip * CORES + to_core, to_sub, to_dp),
                        )
                    else:
                        pltpu.make_async_copy(src, dst, cg_recv.at[slot]).start()
    hand_out(2, key_acc[:span].astype(jnp.bfloat16), key_grad)
    hand_out(3, value_acc[:span].astype(jnp.bfloat16), value_grad)

    collect(0, attended)
    collect(1, query_grad)
    collect(2, key_grad)
    collect(3, value_grad)
    for slot in range(2):
        if direct:
            wait_bytes(coarse_out[slot], cg_recv.at[slot])
            wait_bytes(coarse_stage.at[slot, : coarse_span - mine], cg_send.at[slot])
        else:
            collect(4 + slot, coarse_out[slot])
    for index, (buffer, size, send) in enumerate(
        ((kv, span, kv_send), (ckv, coarse_span, c_send), (qg, span, qg_send))
    ):
        for hop in range(chips - 1):
            for right in (0, 1):
                at = chip - hop if right else chip + hop
                had = jnp.logical_and(at >= 0, chip + 1 < chips) if right else jnp.logical_and(
                    at < chips, chip >= 1
                )
                block = buffer.at[:, block_of(chip, size)]
                pl.when(had)(
                    lambda block=block, sem=send.at[right, hop]: wait_bytes(block, sem)
                )
    wait_bytes(kv.at[:, my_rows], near_send.at[0])
    wait_bytes(qg.at[:, my_rows], near_send.at[1])
    wait_bytes(ckv.at[:, : coarse_span - mine], near_send.at[2])
    wait_bytes(stats.at[: chips - 1], stat_send)


def fused(sizes, queries, keys, values, out_grad, coarse_keys, coarse_values, fine_scale, direct):
    n_fine, n_sub, n_dp = sizes
    rows, width = queries.shape[1:]
    total = rows * n_fine
    chips, span = n_fine // CORES, rows * CORES
    coarse_total = coarse_keys.shape[1] * n_fine * (n_sub * n_dp if direct else 1)
    coarse_span = coarse_total // chips
    bf16, f32 = jnp.bfloat16, jnp.float32
    hbm_spec = pl.BlockSpec(memory_space=pltpu.HBM)
    vmem_spec = pl.BlockSpec(memory_space=pltpu.VMEM)
    dma = pltpu.SemaphoreType.DMA
    return pl.pallas_call(
        functools.partial(kernel, sizes, direct),
        out_shape=[jax.ShapeDtypeStruct(queries.shape, bf16)] * 4
        + [jax.ShapeDtypeStruct(coarse_keys.shape, bf16)] * 2,
        in_specs=[hbm_spec] * 7,
        out_specs=[vmem_spec] * 6,
        scratch_shapes=[
            pltpu.VMEM((1, fine_scale.shape[0]), jnp.int32),
            pltpu.VMEM((2, rows, width), bf16),
            pltpu.VMEM((2, rows, width), bf16),
            pltpu.VMEM((2,) + coarse_keys.shape, bf16),
            pltpu.VMEM((2, total, HEAD), bf16),
            pltpu.VMEM((2, total, HEAD), bf16),
            pltpu.VMEM((2, coarse_total, HEAD), bf16),
            pltpu.VMEM((chips, 8, span), f32),
            pltpu.VMEM((6, span, HEAD), bf16),
            pltpu.VMEM((2, coarse_span, HEAD), bf16),
            pltpu.VMEM((span + coarse_span, HEAD), f32),
            pltpu.VMEM((span + coarse_span, HEAD), f32),
            dma((7,)),
            dma((chips,)),
            dma((chips,)),
            dma((chips,)),
            dma((chips,)),
            dma((6,)),
            dma((2,)),
            dma((2, chips)),
            dma((2, chips)),
            dma((2, chips)),
            dma((3,)),
            dma,
            dma((6,)),
            dma((2,)),
        ],
        compiler_params=pltpu.CompilerParams(
            collective_id=0, has_side_effects=True, vmem_limit_bytes=48 * 1024 * 1024
        ),
    )(
        *(
            pltpu.with_memory_space_constraint(argument, pltpu.HBM)
            for argument in (
                queries,
                keys,
                values,
                out_grad,
                coarse_keys,
                coarse_values,
                fine_scale.reshape(1, fine_scale.shape[0]),
            )
        )
    )


def host_kernel(
    sizes,
    queries,
    keys,
    values,
    out_grad,
    coarse_keys,
    coarse_values,
    scale_in,
    attended,
    query_grad,
    key_grad,
    value_grad,
    coarse_key_grad,
    coarse_value_grad,
    scale_row,
    kv_src,
    qg_src,
    c_src,
    plane_in,
    kv,
    qg,
    stage,
    key_acc,
    value_acc,
    swap_out,
    swap_in,
    total_out,
    load_sem,
    own_sem,
    plane_recv,
    kv_recv,
    c_recv,
    qg_recv,
    near_recv,
    swap_recv,
    out_recv,
    coarse_recv,
    plane_send,
    kv_send,
    c_send,
    qg_send,
    near_send,
    swap_send,
    row_send,
    key_send,
    coarse_send,
):
    n_fine, n_sub, n_dp = sizes
    fine, sub, dp = lax.axis_index("fine"), lax.axis_index("sub"), lax.axis_index("dp")
    chip, core = fine // CORES, lax.rem(fine, CORES)
    chips = n_fine // CORES
    first_host = chips // 2 - 1
    heads = queries.shape[2] // HEAD
    rows = keys.shape[1]
    mine = coarse_keys.shape[1]
    crows = mine * n_sub * n_dp
    half, chalf = chips * rows, chips * crows
    fines = CORES * half
    partner = {"fine": chip * CORES + (1 - core)}
    unit = chip - first_host
    hosting = jnp.logical_and(unit >= 0, unit < heads)
    left = chip < chips // 2

    def head_columns(index, count=1):
        return pl.ds(pl.multiple_of(index * HEAD, HEAD), count * HEAD)

    def block_of(at, size):
        return pl.ds(pl.multiple_of(at * size, size), size)

    def fine_rows(owner, at):
        return block_of(owner * chips + at, rows)

    def coarse_rows(owner, at):
        return pl.ds(pl.multiple_of(fines + (owner * chips + at) * crows, crows), crows)

    def load(src, dst, sem):
        copy = pltpu.make_async_copy(src, dst, sem)
        copy.start()
        return copy

    def remote(src, dst, send, recv, device):
        pltpu.make_async_remote_copy(
            src_ref=src,
            dst_ref=dst,
            send_sem=send,
            recv_sem=recv,
            device_id=device,
            device_id_type=MESH,
        ).start()

    my_slot = sub * n_dp + dp
    loads = [
        load(src, dst, load_sem.at[slot])
        for slot, (src, dst) in enumerate(
            (
                (coarse_keys, c_src.at[0]),
                (coarse_values, c_src.at[1]),
                (keys.at[0], kv_src.at[0]),
                (values.at[0], kv_src.at[1]),
                (queries.at[0], qg_src.at[0]),
                (out_grad.at[0], qg_src.at[1]),
                (scale_in, scale_row),
                (
                    coarse_keys.at[dp, :, head_columns(sub * heads, heads)],
                    plane_in.at[0, block_of(my_slot, mine)],
                ),
                (
                    coarse_values.at[dp, :, head_columns(sub * heads, heads)],
                    plane_in.at[1, block_of(my_slot, mine)],
                ),
            )
        )
    ]
    own_pairs = (
        (keys, kv.at[0, fine_rows(core, chip)]),
        (values, kv.at[1, fine_rows(core, chip)]),
        (queries, qg.at[0, block_of(chip, rows)]),
        (out_grad, qg.at[1, block_of(chip, rows)]),
    )

    @pl.when(hosting)
    def _():
        for slot, (src, dst) in enumerate(own_pairs):
            load(src.at[0, :, head_columns(unit)], dst, own_sem.at[slot])

    barrier = pltpu.get_barrier_semaphore()

    def greet(device):
        pl.semaphore_signal(barrier, inc=1, device_id=device, device_id_type=MESH)

    plane = []
    for step_sub in range(n_sub):
        for step_dp in range(n_dp):
            if step_sub or step_dp:
                plane.append((lax.rem(sub + step_sub, n_sub), lax.rem(dp + step_dp, n_dp)))
    for to_sub, to_dp in plane:
        greet((fine, to_sub, to_dp))
    pl.when(hosting)(lambda: greet((partner["fine"], sub, dp)))
    for step in range(1, chips):
        to = lax.rem(chip + step, chips)
        to_host = jnp.logical_and(to >= first_host, to < first_host + heads)
        pl.when(jnp.logical_or(hosting, to_host))(
            lambda to=to: greet((to * CORES + core, sub, dp))
        )
    pl.semaphore_wait(barrier, len(plane) + jnp.where(hosting, chips, heads))

    for at in (0, 1):
        loads[at].wait()
    for index, (to_sub, to_dp) in enumerate(plane):
        remote(
            c_src.at[:, to_dp, :, head_columns(to_sub * heads, heads)],
            plane_in.at[:, block_of(my_slot, mine)],
            plane_send.at[index],
            plane_recv,
            (fine, to_sub, to_dp),
        )

    def to_hosts(far_first, src, dst, send, recv):
        for step in range(heads):
            nth = jnp.where(left, step, heads - 1 - step)
            head = heads - 1 - nth if far_first else nth
            host = first_host + head
            pl.when(host != chip)(
                lambda head=head, host=host: remote(
                    src.at[:, :, head_columns(head)],
                    dst,
                    send.at[head],
                    recv.at[chip],
                    {"fine": host * CORES + core},
                )
            )

    for at in (2, 3):
        loads[at].wait()
    to_hosts(True, kv_src, kv.at[:, fine_rows(core, chip)], kv_send, kv_recv)
    for at in (7, 8):
        loads[at].wait()
    wait_bytes(plane_in.at[:, : crows - mine], plane_recv)
    to_hosts(True, plane_in, kv.at[:, coarse_rows(core, chip)], c_send, c_recv)
    for at in (4, 5):
        loads[at].wait()
    to_hosts(False, qg_src, qg.at[:, block_of(chip, rows)], qg_send, qg_recv)
    loads[6].wait()

    outs = (attended, query_grad, key_grad, value_grad)
    coarse_outs = (coarse_key_grad, coarse_value_grad)

    @pl.when(hosting)
    def _():
        columns = head_columns(unit)
        away = jnp.where(unit == 0, 1, -1)
        offsets = [0]
        for reach in range(1, chips // 2 + 1):
            offsets += [reach, -reach]
        offsets = offsets[:chips]
        order = [chip + away * offset for offset in offsets]

        def pass_near(block, index):
            remote(block, block, near_send.at[index], near_recv.at[index], partner)

        for index, (src, dst) in enumerate(own_pairs):
            pltpu.make_async_copy(src.at[0, :, columns], dst, own_sem.at[index]).wait()
        pass_near(kv.at[:, fine_rows(core, chip)], 0)
        own_coarse = plane_in.at[:, :, columns]
        remote(
            own_coarse,
            kv.at[:, coarse_rows(core, chip)],
            near_send.at[chips],
            near_recv.at[chips],
            partner,
        )
        kv[:, coarse_rows(core, chip)] = own_coarse[...]
        for index, at in list(enumerate(order))[1:]:
            block = kv.at[:, fine_rows(core, at)]
            wait_bytes(block, kv_recv.at[at])
            pass_near(block, index)
        for index, at in list(enumerate(order))[1:]:
            block = kv.at[:, coarse_rows(core, at)]
            wait_bytes(block, c_recv.at[at])
            pass_near(block, chips + index)

        key_scale = jnp.concatenate(
            [
                scale_row[:, (at * CORES + owner) * rows : (at * CORES + owner + 1) * rows]
                for owner in range(CORES)
                for at in range(chips)
            ],
            axis=1,
        )
        for index, at in enumerate(order):
            wait_bytes(kv.at[:, fine_rows(1 - core, at)], near_recv.at[index])
        for index, at in enumerate(order):
            wait_bytes(kv.at[:, coarse_rows(1 - core, at)], near_recv.at[chips + index])

        for index, at in enumerate(order):
            block_rows = block_of(at, rows)
            if index:
                wait_bytes(qg.at[:, block_rows], qg_recv.at[at])
            query, grad = qg[0, block_rows], qg[1, block_rows]
            own_scale = scale_row[:, block_of(at * CORES + core, rows)]
            own_column = jnp.transpose(jnp.broadcast_to(own_scale, (HEAD, rows)))[:, :1]
            scores = nt(query, kv[0])
            scores = jnp.concatenate(
                [
                    jnp.where(key_scale <= own_column, scores[:, :fines], -jnp.inf),
                    scores[:, fines:],
                ],
                axis=1,
            )
            peak = jnp.max(scores, axis=1, keepdims=True)
            powers = jnp.exp((scores - peak) * INVERSE)
            scale = 1.0 / jnp.sum(powers, axis=1, keepdims=True)
            weights = powers * scale
            dots = nt(grad, kv[1])
            delta = jnp.sum(weights * dots, axis=1, keepdims=True)
            weights = weights.astype(jnp.bfloat16)
            grads = (weights.astype(jnp.float32) * (dots - delta) * INVERSE).astype(jnp.bfloat16)
            out = nn(weights, kv[1]).astype(jnp.bfloat16)
            query_out = nn(grads, kv[0]).astype(jnp.bfloat16)
            for slot, value in enumerate((out, query_out)):
                if not index:
                    outs[slot][0, :, columns] = value
                    continue
                stage[slot, index - 1] = value
                remote(
                    stage.at[slot, index - 1],
                    outs[slot].at[0, :, columns],
                    row_send.at[slot, index - 1],
                    out_recv.at[slot, unit],
                    {"fine": at * CORES + core},
                )
            value_part, key_part = tn(weights, grad), tn(grads, query)
            if index:
                value_part += value_acc[...]
                key_part += key_acc[...]
            value_acc[...] = value_part
            key_acc[...] = key_part

        accs = (key_acc, value_acc)
        for slot in (1, 0):
            swap_out[slot, :half] = accs[slot][block_of(1 - core, half)].astype(jnp.bfloat16)
            swap_out[slot, half:] = accs[slot][
                pl.ds(pl.multiple_of(fines + (1 - core) * chalf, chalf), chalf)
            ].astype(jnp.bfloat16)
            remote(
                swap_out.at[slot], swap_in.at[slot], swap_send.at[slot], swap_recv.at[slot], partner
            )
        for slot in (1, 0):
            wait_bytes(swap_in.at[slot], swap_recv.at[slot])
            total_out[slot, :half] = (
                accs[slot][block_of(core, half)] + swap_in[slot, :half].astype(jnp.float32)
            ).astype(jnp.bfloat16)
            total_out[slot, half:] = (
                accs[slot][pl.ds(pl.multiple_of(fines + core * chalf, chalf), chalf)]
                + swap_in[slot, half:].astype(jnp.float32)
            ).astype(jnp.bfloat16)
            result = outs[2 + slot]
            for index, at in reversed(list(enumerate(order))):
                block = total_out.at[slot, block_of(at, rows)]
                if index:
                    remote(
                        block,
                        result.at[0, :, columns],
                        key_send.at[slot, index - 1],
                        out_recv.at[2 + slot, unit],
                        {"fine": at * CORES + core},
                    )
                else:
                    result[0, :, columns] = block[...]
                for to_sub, to_dp in [(sub, dp)] + plane:
                    piece = (at * n_sub + to_sub) * n_dp + to_dp
                    src = total_out.at[
                        slot, pl.ds(pl.multiple_of(half + piece * mine, mine), mine)
                    ]
                    dst = coarse_outs[slot].at[dp, :, head_columns(sub * heads + unit)]
                    if index == 0 and to_sub is sub and to_dp is dp:
                        pltpu.make_async_copy(src, dst, coarse_recv.at[slot]).start()
                    else:
                        remote(
                            src,
                            dst,
                            coarse_send.at[slot],
                            coarse_recv.at[slot],
                            (at * CORES + core, to_sub, to_dp),
                        )

    for head in range(heads):

        @pl.when(first_host + head != chip)
        def _(head=head):
            for slot, result in enumerate(outs):
                wait_bytes(
                    result.at[0, :, head * HEAD : (head + 1) * HEAD], out_recv.at[slot, head]
                )

    for slot, result in enumerate(coarse_outs):
        wait_bytes(result, coarse_recv.at[slot])
    for index in range(len(plane)):
        wait_bytes(c_src.at[:, 0, :, : heads * HEAD], plane_send.at[index])
    for head in range(heads):

        @pl.when(first_host + head != chip)
        def _(head=head):
            wait_bytes(kv_src.at[:, :, :HEAD], kv_send.at[head])
            wait_bytes(plane_in.at[:, :, :HEAD], c_send.at[head])
            wait_bytes(qg_src.at[:, :, :HEAD], qg_send.at[head])

    @pl.when(hosting)
    def _():
        for index in range(chips):
            wait_bytes(kv.at[:, :rows], near_send.at[index])
            wait_bytes(kv.at[:, fines : fines + crows], near_send.at[chips + index])
        for slot in range(2):
            wait_bytes(swap_out.at[slot], swap_send.at[slot])
            for index in range(chips - 1):
                wait_bytes(stage.at[slot, index], row_send.at[slot, index])
                wait_bytes(total_out.at[slot, :rows], key_send.at[slot, index])
            wait_bytes(total_out.at[slot, : chalf - mine], coarse_send.at[slot])


def fits_hosts(sizes, queries):
    chips, heads = sizes[0] // CORES, queries.shape[2] // HEAD
    return heads == CORES and chips % 2 == 0 and chips <= 2 * CORES


def hosted(sizes, queries, keys, values, out_grad, coarse_keys, coarse_values, fine_scale):
    n_fine, n_sub, n_dp = sizes
    rows, width = queries.shape[1:]
    heads, chips, mine = width // HEAD, n_fine // CORES, coarse_keys.shape[1]
    crows = mine * n_sub * n_dp
    half = chips * (rows + crows)
    total = CORES * half
    bf16, f32 = jnp.bfloat16, jnp.float32
    dma = pltpu.SemaphoreType.DMA
    return pl.pallas_call(
        functools.partial(host_kernel, sizes),
        out_shape=[jax.ShapeDtypeStruct(queries.shape, bf16)] * 4
        + [jax.ShapeDtypeStruct(coarse_keys.shape, bf16)] * 2,
        in_specs=[pl.BlockSpec(memory_space=pltpu.HBM)] * 7,
        out_specs=[pl.BlockSpec(memory_space=pltpu.VMEM)] * 6,
        scratch_shapes=[
            pltpu.VMEM((1, fine_scale.shape[0]), jnp.int32),
            pltpu.VMEM((2, rows, width), bf16),
            pltpu.VMEM((2, rows, width), bf16),
            pltpu.VMEM((2,) + coarse_keys.shape, bf16),
            pltpu.VMEM((2, crows, width), bf16),
            pltpu.VMEM((2, total, HEAD), bf16),
            pltpu.VMEM((2, chips * rows, HEAD), bf16),
            pltpu.VMEM((2, chips - 1, rows, HEAD), bf16),
            pltpu.VMEM((total, HEAD), f32),
            pltpu.VMEM((total, HEAD), f32),
            pltpu.VMEM((2, half, HEAD), bf16),
            pltpu.VMEM((2, half, HEAD), bf16),
            pltpu.VMEM((2, half, HEAD), bf16),
            dma((9,)),
            dma((4,)),
            dma,
            dma((chips,)),
            dma((chips,)),
            dma((chips,)),
            dma((2 * chips,)),
            dma((2,)),
            dma((4, heads)),
            dma((2,)),
            dma((n_sub * n_dp - 1,)),
            dma((heads,)),
            dma((heads,)),
            dma((heads,)),
            dma((2 * chips,)),
            dma((2,)),
            dma((2, chips - 1)),
            dma((2, chips - 1)),
            dma((2,)),
        ],
        compiler_params=pltpu.CompilerParams(
            collective_id=0, has_side_effects=True, vmem_limit_bytes=48 * 1024 * 1024
        ),
    )(
        *(
            pltpu.with_memory_space_constraint(argument, pltpu.HBM)
            for argument in (
                queries,
                keys,
                values,
                out_grad,
                coarse_keys,
                coarse_values,
                fine_scale.reshape(1, fine_scale.shape[0]),
            )
        )
    )


def place(count, *refs):
    sem = refs[2 * count]
    stores = [
        pltpu.make_async_copy(refs[i], refs[count + i], sem.at[i]) for i in range(count)
    ]
    for store in stores:
        store.start()
    for store in stores:
        store.wait()


def placed_out(results):
    count = len(results)
    return pl.pallas_call(
        functools.partial(place, count),
        out_shape=[jax.ShapeDtypeStruct(result.shape, result.dtype) for result in results],
        in_specs=[pl.BlockSpec(memory_space=pltpu.VMEM)] * count,
        out_specs=[pl.BlockSpec(memory_space=pltpu.HBM)] * count,
        scratch_shapes=[pltpu.SemaphoreType.DMA((count,))],
        compiler_params=pltpu.CompilerParams(vmem_limit_bytes=8 * 1024 * 1024),
    )(*results)


def shards(sizes, queries, keys, values, out_grad, coarse_keys, coarse_values, fine_scale):
    direct = coarse_keys.shape[1] % 16 == 0
    fine = (queries, keys, values, out_grad)
    if direct:
        call = hosted if fits_hosts(sizes, queries) else functools.partial(fused, direct=True)
        return tuple(placed_out(call(sizes, *fine, coarse_keys, coarse_values, fine_scale)))

    def gathered(coarse):
        image = lax.all_to_all(coarse, "dp", split_axis=0, concat_axis=1, tiled=True)
        return lax.all_to_all(image, "sub", split_axis=2, concat_axis=1, tiled=True)

    def returned(grad):
        back = lax.all_to_all(grad, "sub", split_axis=1, concat_axis=2, tiled=True)
        return lax.all_to_all(back, "dp", split_axis=1, concat_axis=0, tiled=True)

    results = fused(
        sizes, *fine, gathered(coarse_keys), gathered(coarse_values), fine_scale, direct=False
    )
    return tuple(results[:4]) + (returned(results[4]), returned(results[5]))


def solution(mesh):
    sizes = tuple(mesh.shape[name] for name in ("fine", "sub", "dp"))
    placed = P("dp", "fine", "sub")
    coarse = P(None, ("fine", "sub", "dp"), None)
    return jax.shard_map(
        functools.partial(shards, sizes),
        mesh=mesh,
        in_specs=(placed,) * 4 + (coarse, coarse, P()),
        out_specs=(placed,) * 4 + (coarse, coarse),
        check_vma=False,
    )
```

```python
import functools
import math

import jax
import jax.numpy as jnp
from jax import lax
from jax.experimental import pallas as pl
from jax.experimental.pallas import tpu as pltpu
from jax.sharding import PartitionSpec as P

HEAD = 128
CORES = 2
MESH = pl.DeviceIdType.MESH
INVERSE = 1.0 / math.sqrt(HEAD)
LOG2E = math.log2(math.e)


def nt(a, b):
    return lax.dot_general(a, b, (((1,), (1,)), ((), ())), preferred_element_type=jnp.float32)


def tn(a, b):
    return lax.dot_general(a, b, (((0,), (0,)), ((), ())), preferred_element_type=jnp.float32)


def nn(a, b):
    return jnp.dot(a, b, preferred_element_type=jnp.float32)


def wait_bytes(ref, sem):
    pltpu.make_async_copy(ref, ref, sem).wait()


def kernel(
    sizes,
    direct,
    queries,
    keys,
    values,
    out_grad,
    coarse_keys,
    coarse_values,
    scale_in,
    attended,
    query_grad,
    key_grad,
    value_grad,
    coarse_key_grad,
    coarse_value_grad,
    scale_row,
    kv_src,
    qg_src,
    c_src,
    kv,
    qg,
    ckv,
    stats,
    stage,
    coarse_stage,
    key_acc,
    value_acc,
    load_sem,
    kv_recv,
    c_recv,
    qg_recv,
    stat_recv,
    out_recv,
    cg_recv,
    kv_send,
    c_send,
    qg_send,
    near_send,
    stat_send,
    out_send,
    cg_send,
):
    n_fine, n_sub, n_dp = sizes
    fine, sub, dp = lax.axis_index("fine"), lax.axis_index("sub"), lax.axis_index("dp")
    chip, core = fine // CORES, lax.rem(fine, CORES)
    chips = n_fine // CORES
    rows = keys.shape[1]
    span = rows * CORES
    coarse_rows = ckv.shape[1]
    coarse_span = coarse_rows // chips
    partner = {"fine": chip * CORES + (1 - core)}

    loads = []
    for slot, (src, dst) in enumerate(
        (
            (keys.at[0], kv_src.at[0]),
            (values.at[0], kv_src.at[1]),
            (coarse_keys, c_src.at[0]),
            (coarse_values, c_src.at[1]),
            (queries.at[0], qg_src.at[0]),
            (out_grad.at[0], qg_src.at[1]),
            (scale_in, scale_row),
        )
    ):
        copy = pltpu.make_async_copy(src, dst, load_sem.at[slot])
        copy.start()
        loads.append(copy)

    barrier = pltpu.get_barrier_semaphore()
    plane = []
    for step_core in range(CORES):
        for step_sub in range(n_sub if direct else 1):
            for step_dp in range(n_dp if direct else 1):
                if step_core or step_sub or step_dp:
                    plane.append(
                        (
                            chip * CORES + lax.rem(core + step_core, CORES),
                            lax.rem(sub + step_sub, n_sub),
                            lax.rem(dp + step_dp, n_dp),
                        )
                    )
    column = []
    for step_chip in range(1, chips):
        for step_core in range(CORES):
            to_chip = lax.rem(chip + step_chip, chips)
            column.append((to_chip * CORES + lax.rem(core + step_core, CORES), sub, dp))
    for other in column + plane:
        pl.semaphore_signal(barrier, inc=1, device_id=other, device_id_type=MESH)
    pl.semaphore_wait(barrier, len(column + plane))

    def head_columns(index):
        return pl.ds(pl.multiple_of(index * HEAD, HEAD), HEAD)

    my_rows = pl.ds(pl.multiple_of(fine * rows, rows), rows)
    chip_rows = pl.ds(pl.multiple_of(chip * span, span), span)
    chip_coarse = pl.ds(pl.multiple_of(chip * coarse_span, coarse_span), coarse_span)

    def remote(src, dst, send, recv, device):
        pltpu.make_async_remote_copy(
            src_ref=src,
            dst_ref=dst,
            send_sem=send,
            recv_sem=recv,
            device_id=device,
            device_id_type=MESH,
        ).start()

    def towards(right, act):
        to = chip + 1 if right else chip - 1
        pl.when(to < chips if right else to >= 0)(lambda: act(to))

    def send_own(src, dst, send, recv, right):
        def both_cores(to):
            for to_core in range(CORES):
                remote(
                    src.at[:, :, to_core * HEAD : (to_core + 1) * HEAD],
                    dst.at[:, my_rows],
                    send.at[right, 0],
                    recv.at[chip],
                    {"fine": to * CORES + to_core},
                )

        towards(right, both_cores)

    def share(src, dst, near, recv):
        remote(
            src.at[:, :, head_columns(1 - core)], dst.at[:, my_rows], near, recv.at[chip], partner
        )
        pltpu.make_async_copy(
            src.at[:, :, head_columns(core)], dst.at[:, my_rows], recv.at[chip]
        ).start()

    def block_of(at, size):
        return pl.ds(pl.multiple_of(at * size, size), size)

    def pass_on(buffer, size, send, recv, hop, right):
        at = chip - hop if right else chip + hop

        def arrived(to):
            block = buffer.at[:, block_of(at, size)]
            wait_bytes(block, recv.at[at])
            remote(block, block, send.at[right, hop], recv.at[at], {"fine": to * CORES + core})

        pl.when(at >= 0 if right else at < chips)(lambda: towards(right, arrived))

    loads[0].wait()
    loads[1].wait()
    for right in (0, 1):
        send_own(kv_src, kv, kv_send, kv_recv, right)
    share(kv_src, kv, near_send.at[0], kv_recv)
    loads[2].wait()
    loads[3].wait()
    mine = coarse_keys.shape[1]
    if direct:
        block = (fine * n_sub + sub) * n_dp + dp
    else:
        block = fine
    mine_rows = pl.ds(pl.multiple_of(block * mine, mine), mine)

    def coarse_piece(image, index):
        return c_src.at[:, image, :, head_columns(index)]

    for to_fine, to_sub, to_dp in plane:
        to_core = lax.rem(to_fine, CORES)
        piece = coarse_piece(to_dp, to_sub * CORES + to_core) if direct else coarse_piece(0, to_core)
        remote(piece, ckv.at[:, mine_rows], near_send.at[2], c_recv.at[chip], (to_fine, to_sub, to_dp))
    piece = coarse_piece(dp, sub * CORES + core) if direct else coarse_piece(0, core)
    pltpu.make_async_copy(piece, ckv.at[:, mine_rows], c_recv.at[chip]).start()
    loads[4].wait()
    loads[5].wait()
    share(qg_src, qg, near_send.at[1], qg_recv)

    own_coarse = ckv.at[:, chip_coarse]
    wait_bytes(own_coarse, c_recv.at[chip])
    for right in (0, 1):
        towards(
            right,
            lambda to, right=right: remote(
                own_coarse,
                own_coarse,
                c_send.at[right, 0],
                c_recv.at[chip],
                {"fine": to * CORES + core},
            ),
        )
    at_end = jnp.logical_or(chip == 0, chip == chips - 1)
    for hop in range(1, chips):
        for right in (0, 1):
            pass_on(kv, span, kv_send, kv_recv, hop, right)
            pass_on(ckv, coarse_span, c_send, c_recv, hop, right)
            spent = chip == hop - 1 if right else chip == chips - hop
            pl.when(spent)(
                lambda right=right: send_own(qg_src, qg, qg_send, qg_recv, right)
            )
    if chips > 2:
        for right in (0, 1):
            pass_on(qg, span, qg_send, qg_recv, 1, right)
    for step in range(1, chips):
        at = lax.rem(chip + step, chips)

        def last_stop(at=at):
            wait_bytes(kv.at[:, block_of(at, span)], kv_recv.at[at])
            wait_bytes(ckv.at[:, block_of(at, coarse_span)], c_recv.at[at])

        pl.when(at_end)(last_stop)

    loads[6].wait()
    scales = scale_row[...].astype(jnp.float32)
    own_scale = scale_row[:, chip_rows].astype(jnp.float32)
    own_column = jnp.transpose(jnp.broadcast_to(own_scale, (HEAD, span)))[:, :1]

    wait_bytes(qg.at[:, chip_rows], qg_recv.at[chip])
    query_own, grad_own = qg[0, chip_rows], qg[1, chip_rows]
    wait_bytes(kv.at[:, chip_rows], kv_recv.at[chip])
    fine_scores = nt(query_own, kv[0]) * INVERSE
    fine_scores = jnp.where(scales <= own_column, fine_scores, -jnp.inf)
    coarse_scores = nt(query_own, ckv[0]) * INVERSE
    peak = jnp.maximum(
        jnp.max(fine_scores, axis=1, keepdims=True), jnp.max(coarse_scores, axis=1, keepdims=True)
    )
    total = jnp.sum(jnp.exp(fine_scores - peak), axis=1, keepdims=True) + jnp.sum(
        jnp.exp(coarse_scores - peak), axis=1, keepdims=True
    )
    log_total = peak + jnp.log(total)
    fine_weights = jnp.exp(fine_scores - log_total).astype(jnp.bfloat16)
    coarse_weights = jnp.exp(coarse_scores - log_total).astype(jnp.bfloat16)
    for hop in range(2, chips - 1):
        for right in (0, 1):
            pass_on(qg, span, qg_send, qg_recv, hop, right)
    out = (nn(fine_weights, kv[1]) + nn(coarse_weights, ckv[1])).astype(jnp.bfloat16)
    delta = jnp.sum(
        grad_own.astype(jnp.float32) * out.astype(jnp.float32), axis=1, keepdims=True
    )
    log_rows = jnp.transpose(jnp.broadcast_to(log_total, (span, HEAD)))[:8]
    delta_rows = jnp.transpose(jnp.broadcast_to(delta, (span, HEAD)))[:8]
    first = lax.broadcasted_iota(jnp.int32, (8, span), 0) == 0
    stats[chip] = jnp.where(first, log_rows, delta_rows)
    for step in range(1, chips):
        to = lax.rem(chip + step, chips)
        remote(
            stats.at[chip],
            stats.at[chip],
            stat_send,
            stat_recv.at[chip],
            {"fine": to * CORES + core},
        )

    def hand_out(slot, value, result):
        height = value.shape[0] // CORES
        stage[slot, : value.shape[0]] = value
        give = pl.ds(pl.multiple_of((1 - core) * height, height), height)
        keep = pl.ds(pl.multiple_of(core * height, height), height)
        remote(
            stage.at[slot, give],
            result.at[0, :, head_columns(core)],
            out_send.at[slot],
            out_recv.at[slot],
            partner,
        )
        result[0, :, head_columns(core)] = stage[slot, keep]

    def collect(slot, result):
        half = result.at[0, :, head_columns(1 - core)]
        wait_bytes(half, out_recv.at[slot])
        wait_bytes(half, out_send.at[slot])

    hand_out(0, out, attended)

    def grads_of(weights, dots, row_delta):
        return (weights.astype(jnp.float32) * (dots - row_delta) * INVERSE).astype(jnp.bfloat16)

    fine_grads = grads_of(fine_weights, nt(grad_own, kv[1]), delta)
    coarse_grads = grads_of(coarse_weights, nt(grad_own, ckv[1]), delta)
    query_out = nn(fine_grads, kv[0]) + nn(coarse_grads, ckv[0])
    hand_out(1, query_out.astype(jnp.bfloat16), query_grad)

    reach = jnp.minimum(chip, chips - 1 - chip)
    longer = jnp.where(chip > chips - 1 - chip, -1, 1)
    for step in range(chips):
        near = -(step + 1) // 2 if step % 2 else step // 2
        at = chip + jnp.where(step <= 2 * reach, near, longer * (step - reach))
        at_rows = pl.ds(pl.multiple_of(at * span, span), span)
        if step:

            def last_queries(at=at, at_rows=at_rows):
                wait_bytes(qg.at[:, at_rows], qg_recv.at[at])

            pl.when(at_end)(last_queries)
            wait_bytes(stats.at[at], stat_recv.at[at])
        query_block, grad_block = qg[0, at_rows], qg[1, at_rows]
        log_row, delta_row = stats[at, 0:1], stats[at, 1:2]
        block_scale = scale_row[:, at_rows].astype(jnp.float32)
        for part in range(2):
            source, own, low = ((kv, chip_rows, 0), (ckv, chip_coarse, span))[part]
            high = low + (span, coarse_span)[part]
            scores = nt(source[0, own], query_block) * INVERSE
            if part == 0:
                scores = jnp.where(own_column <= block_scale, scores, -jnp.inf)
            weights = jnp.exp(scores - log_row).astype(jnp.bfloat16)
            value_part = nn(weights, grad_block)
            grads = grads_of(weights, nt(source[1, own], grad_block), delta_row)
            key_part = nn(grads, query_block)
            if step:
                value_part += value_acc[low:high]
                key_part += key_acc[low:high]
            value_acc[low:high] = value_part
            key_acc[low:high] = key_part

    coarse_out = (coarse_key_grad, coarse_value_grad)
    for slot, acc in enumerate((key_acc, value_acc)):
        part = acc[span:].astype(jnp.bfloat16)
        if not direct:
            hand_out(4 + slot, part, coarse_out[slot])
            continue
        coarse_stage[slot] = part
        for step_core in range(CORES):
            for step_sub in range(n_sub):
                for step_dp in range(n_dp):
                    to_core = lax.rem(core + step_core, CORES)
                    to_sub = lax.rem(sub + step_sub, n_sub)
                    to_dp = lax.rem(dp + step_dp, n_dp)
                    piece = (to_core * n_sub + to_sub) * n_dp + to_dp
                    src = coarse_stage.at[slot, pl.ds(pl.multiple_of(piece * mine, mine), mine)]
                    dst = coarse_out[slot].at[dp, :, head_columns(sub * CORES + core)]
                    if step_core or step_sub or step_dp:
                        remote(
                            src,
                            dst,
                            cg_send.at[slot],
                            cg_recv.at[slot],
                            (chip * CORES + to_core, to_sub, to_dp),
                        )
                    else:
                        pltpu.make_async_copy(src, dst, cg_recv.at[slot]).start()
    hand_out(2, key_acc[:span].astype(jnp.bfloat16), key_grad)
    hand_out(3, value_acc[:span].astype(jnp.bfloat16), value_grad)

    collect(0, attended)
    collect(1, query_grad)
    collect(2, key_grad)
    collect(3, value_grad)
    for slot in range(2):
        if direct:
            wait_bytes(coarse_out[slot], cg_recv.at[slot])
            wait_bytes(coarse_stage.at[slot, : coarse_span - mine], cg_send.at[slot])
        else:
            collect(4 + slot, coarse_out[slot])
    for index, (buffer, size, send) in enumerate(
        ((kv, span, kv_send), (ckv, coarse_span, c_send), (qg, span, qg_send))
    ):
        for hop in range(chips - 1):
            for right in (0, 1):
                at = chip - hop if right else chip + hop
                had = jnp.logical_and(at >= 0, chip + 1 < chips) if right else jnp.logical_and(
                    at < chips, chip >= 1
                )
                block = buffer.at[:, block_of(chip, size)]
                pl.when(had)(
                    lambda block=block, sem=send.at[right, hop]: wait_bytes(block, sem)
                )
    wait_bytes(kv.at[:, my_rows], near_send.at[0])
    wait_bytes(qg.at[:, my_rows], near_send.at[1])
    wait_bytes(ckv.at[:, : coarse_span - mine], near_send.at[2])
    wait_bytes(stats.at[: chips - 1], stat_send)


def fused(sizes, queries, keys, values, out_grad, coarse_keys, coarse_values, fine_scale, direct):
    n_fine, n_sub, n_dp = sizes
    rows, width = queries.shape[1:]
    total = rows * n_fine
    chips, span = n_fine // CORES, rows * CORES
    coarse_total = coarse_keys.shape[1] * n_fine * (n_sub * n_dp if direct else 1)
    coarse_span = coarse_total // chips
    bf16, f32 = jnp.bfloat16, jnp.float32
    hbm_spec = pl.BlockSpec(memory_space=pltpu.HBM)
    vmem_spec = pl.BlockSpec(memory_space=pltpu.VMEM)
    dma = pltpu.SemaphoreType.DMA
    return pl.pallas_call(
        functools.partial(kernel, sizes, direct),
        out_shape=[jax.ShapeDtypeStruct(queries.shape, bf16)] * 4
        + [jax.ShapeDtypeStruct(coarse_keys.shape, bf16)] * 2,
        in_specs=[hbm_spec] * 7,
        out_specs=[vmem_spec] * 6,
        scratch_shapes=[
            pltpu.VMEM((1, fine_scale.shape[0]), jnp.int32),
            pltpu.VMEM((2, rows, width), bf16),
            pltpu.VMEM((2, rows, width), bf16),
            pltpu.VMEM((2,) + coarse_keys.shape, bf16),
            pltpu.VMEM((2, total, HEAD), bf16),
            pltpu.VMEM((2, total, HEAD), bf16),
            pltpu.VMEM((2, coarse_total, HEAD), bf16),
            pltpu.VMEM((chips, 8, span), f32),
            pltpu.VMEM((6, span, HEAD), bf16),
            pltpu.VMEM((2, coarse_span, HEAD), bf16),
            pltpu.VMEM((span + coarse_span, HEAD), f32),
            pltpu.VMEM((span + coarse_span, HEAD), f32),
            dma((7,)),
            dma((chips,)),
            dma((chips,)),
            dma((chips,)),
            dma((chips,)),
            dma((6,)),
            dma((2,)),
            dma((2, chips)),
            dma((2, chips)),
            dma((2, chips)),
            dma((3,)),
            dma,
            dma((6,)),
            dma((2,)),
        ],
        compiler_params=pltpu.CompilerParams(
            collective_id=0, has_side_effects=True, vmem_limit_bytes=48 * 1024 * 1024
        ),
    )(
        *(
            pltpu.with_memory_space_constraint(argument, pltpu.HBM)
            for argument in (
                queries,
                keys,
                values,
                out_grad,
                coarse_keys,
                coarse_values,
                fine_scale.reshape(1, fine_scale.shape[0]),
            )
        )
    )


def host_kernel(
    sizes,
    queries,
    keys,
    values,
    out_grad,
    coarse_keys,
    coarse_values,
    scale_in,
    attended,
    query_grad,
    key_grad,
    value_grad,
    coarse_key_grad,
    coarse_value_grad,
    scale_row,
    kv_src,
    qg_src,
    c_src,
    plane_in,
    kv,
    flipped,
    qg,
    stage,
    key_acc,
    value_acc,
    swap_out,
    swap_in,
    total_out,
    load_sem,
    own_sem,
    plane_recv,
    kv_recv,
    c_recv,
    qg_recv,
    near_recv,
    swap_recv,
    out_recv,
    coarse_recv,
    plane_send,
    kv_send,
    c_send,
    qg_send,
    near_send,
    swap_send,
    row_send,
    key_send,
    coarse_send,
):
    n_fine, n_sub, n_dp = sizes
    fine, sub, dp = lax.axis_index("fine"), lax.axis_index("sub"), lax.axis_index("dp")
    chip, core = fine // CORES, lax.rem(fine, CORES)
    chips = n_fine // CORES
    first_host = chips // 2 - 1
    heads = queries.shape[2] // HEAD
    rows = keys.shape[1]
    mine = coarse_keys.shape[1]
    crows = mine * n_sub * n_dp
    half = chips * rows
    share = half + chips * crows
    partner = {"fine": chip * CORES + (1 - core)}
    unit = chip - first_host
    hosting = jnp.logical_and(unit >= 0, unit < heads)
    left = chip < chips // 2

    def head_columns(index, count=1):
        return pl.ds(pl.multiple_of(index * HEAD, HEAD), count * HEAD)

    def block_of(at, size):
        return pl.ds(pl.multiple_of(at * size, size), size)

    def fine_rows(part, at):
        return pl.ds(pl.multiple_of(part * share + at * rows, rows), rows)

    def coarse_rows(part, at):
        return pl.ds(pl.multiple_of(part * share + half + at * crows, crows), crows)

    def load(src, dst, sem):
        copy = pltpu.make_async_copy(src, dst, sem)
        copy.start()
        return copy

    def remote(src, dst, send, recv, device):
        pltpu.make_async_remote_copy(
            src_ref=src,
            dst_ref=dst,
            send_sem=send,
            recv_sem=recv,
            device_id=device,
            device_id_type=MESH,
        ).start()

    my_slot = sub * n_dp + dp
    loads = [
        load(src, dst, load_sem.at[slot])
        for slot, (src, dst) in enumerate(
            (
                (coarse_keys, c_src.at[0]),
                (coarse_values, c_src.at[1]),
                (keys.at[0], kv_src.at[0]),
                (values.at[0], kv_src.at[1]),
                (queries.at[0], qg_src.at[0]),
                (out_grad.at[0], qg_src.at[1]),
                (scale_in, scale_row),
                (
                    coarse_keys.at[dp, :, head_columns(sub * heads, heads)],
                    plane_in.at[0, block_of(my_slot, mine)],
                ),
                (
                    coarse_values.at[dp, :, head_columns(sub * heads, heads)],
                    plane_in.at[1, block_of(my_slot, mine)],
                ),
            )
        )
    ]
    own_pairs = (
        (keys, kv.at[0, fine_rows(0, chip)]),
        (values, kv.at[1, fine_rows(0, chip)]),
        (queries, qg.at[0, block_of(chip, rows)]),
        (out_grad, qg.at[1, block_of(chip, rows)]),
    )

    @pl.when(hosting)
    def _():
        for slot, (src, dst) in enumerate(own_pairs):
            load(src.at[0, :, head_columns(unit)], dst, own_sem.at[slot])

    barrier = pltpu.get_barrier_semaphore()

    def greet(device):
        pl.semaphore_signal(barrier, inc=1, device_id=device, device_id_type=MESH)

    plane = []
    for step_sub in range(n_sub):
        for step_dp in range(n_dp):
            if step_sub or step_dp:
                plane.append((lax.rem(sub + step_sub, n_sub), lax.rem(dp + step_dp, n_dp)))
    for to_sub, to_dp in plane:
        greet((fine, to_sub, to_dp))
    pl.when(hosting)(lambda: greet((partner["fine"], sub, dp)))
    for step in range(1, chips):
        to = lax.rem(chip + step, chips)
        pl.when(hosting)(lambda to=to: greet((to * CORES + core, sub, dp)))
    pl.semaphore_wait(barrier, len(plane) + heads)

    for at in (0, 1):
        loads[at].wait()
    for index, (to_sub, to_dp) in enumerate(plane):
        remote(
            c_src.at[:, to_dp, :, head_columns(to_sub * heads, heads)],
            plane_in.at[:, block_of(my_slot, mine)],
            plane_send.at[index],
            plane_recv,
            (fine, to_sub, to_dp),
        )

    def to_host(nth, src, dst, send, recv):
        head = jnp.where(left, nth, heads - 1 - nth)
        host = first_host + head
        pl.when(host != chip)(
            lambda: remote(
                src.at[:, :, head_columns(head)],
                dst,
                send.at[head],
                recv.at[chip],
                {"fine": host * CORES + core},
            )
        )

    def give_queries(nth):
        to_host(nth, qg_src, qg.at[:, block_of(chip, rows)], qg_send, qg_recv)

    near_to_far = range(heads)
    for at in (2, 3):
        loads[at].wait()
    for nth in reversed(near_to_far):
        to_host(nth, kv_src, kv.at[:, fine_rows(0, chip)], kv_send, kv_recv)
    for at in (4, 5):
        loads[at].wait()
    pl.when(left)(lambda: give_queries(heads - 1))
    for at in (7, 8):
        loads[at].wait()
    wait_bytes(plane_in.at[:, : crows - mine], plane_recv)
    for nth in reversed(near_to_far):
        to_host(nth, plane_in, kv.at[:, coarse_rows(0, chip)], c_send, c_recv)
    for nth in near_to_far[:-1]:
        give_queries(nth)
    pl.when(jnp.logical_not(left))(lambda: give_queries(heads - 1))
    loads[6].wait()

    outs = (attended, query_grad, key_grad, value_grad)
    coarse_outs = (coarse_key_grad, coarse_value_grad)
    accs = (key_acc, value_acc)

    @pl.when(hosting)
    def _():
        columns = head_columns(unit)
        other_host = 2 * first_host + 1 - chip
        others, given = [other_host], [other_host]
        if chips > CORES:
            first, last_end = 0 * chip, 0 * chip + chips - 1
            pick = functools.partial(jnp.where, unit == 0)
            others = [pick(other_host, first), pick(first, other_host), last_end]
            given = [first, last_end, other_host]
        order = [chip] + others

        def pass_near(block, dst, index):
            remote(block, dst, near_send.at[index], near_recv.at[index], partner)

        for index, (src, dst) in enumerate(own_pairs):
            pltpu.make_async_copy(src.at[0, :, columns], dst, own_sem.at[index]).wait()
        own_coarse = plane_in.at[:, :, columns]
        pass_near(kv.at[:, fine_rows(0, chip)], kv.at[:, fine_rows(1, chip)], 0)
        pass_near(own_coarse, kv.at[:, coarse_rows(1, chip)], chips)
        kv[:, coarse_rows(0, chip)] = own_coarse[...]
        for index, at in enumerate(others):
            block = kv.at[:, fine_rows(0, at)]
            wait_bytes(block, kv_recv.at[at])
            pass_near(block, kv.at[:, fine_rows(1, at)], 1 + index)

        def flip(low, high):
            for slot in range(2):
                flipped[slot, :, low:high] = jnp.transpose(kv[slot, low:high])

        flip(0, half)
        for index, at in enumerate(others):
            block = kv.at[:, coarse_rows(0, at)]
            wait_bytes(block, c_recv.at[at])
            pass_near(block, kv.at[:, coarse_rows(1, at)], chips + 1 + index)
        flip(half, share)
        for step, source in enumerate(order):
            wait_bytes(kv.at[:, fine_rows(1, source)], near_recv.at[step])
        flip(share, share + half)
        for step, source in enumerate(order):
            wait_bytes(kv.at[:, coarse_rows(1, source)], near_recv.at[chips + step])
        flip(share + half, CORES * share)

        def scales_of(owner):
            return jnp.concatenate(
                [scale_row[:, block_of(at * CORES + owner, rows)] for at in range(chips)], axis=1
            )

        key_scales = (scales_of(core), scales_of(1 - core))
        groups = [range(low, low + 2) for low in range(0, chips, 2)]
        for turn, group in enumerate(groups):
            last = turn + 1 == len(groups)
            for index in group:
                if index:
                    wait_bytes(qg.at[:, block_of(order[index], rows)], qg_recv.at[order[index]])
            query, grad = [
                jnp.concatenate([qg[slot, block_of(order[index], rows)] for index in group])
                for slot in range(2)
            ]
            own_scale = jnp.concatenate(
                [scale_row[:, block_of(order[index] * CORES + core, rows)] for index in group],
                axis=1,
            )
            own_column = jnp.transpose(
                jnp.broadcast_to(own_scale, (HEAD, len(group) * rows))
            )[:, :1]
            scores = nn(query, flipped[0])
            pieces = []
            for part in range(CORES):
                low = part * share
                pieces += [
                    jnp.where(
                        key_scales[part] <= own_column, scores[:, low : low + half], -jnp.inf
                    ),
                    scores[:, low + half : low + share],
                ]
            scores = jnp.concatenate(pieces, axis=1)
            dots = nn(grad, flipped[1])
            peak = jnp.max(scores, axis=1, keepdims=True)
            powers = jnp.exp2((scores - peak) * (INVERSE * LOG2E))
            scale = 1.0 / jnp.sum(powers, axis=1, keepdims=True)
            delta = jnp.sum(powers * dots, axis=1, keepdims=True) * scale
            slope = scale * INVERSE
            powers = powers.astype(jnp.bfloat16)
            grads = powers * (dots - delta).astype(jnp.bfloat16)
            sides = ((grads, query, slope), (powers, grad, scale))
            for slot in (1, 0):
                right_side, rows_in, factor = sides[slot]
                scaled = (rows_in.astype(jnp.float32) * factor).astype(jnp.bfloat16)
                value = nn(jnp.transpose(scaled), right_side)
                if turn:
                    value += accs[slot][...]
                if not last:
                    accs[slot][...] = value
                    continue
                swap_out[slot] = value[:, share:].astype(jnp.bfloat16)
                remote(
                    swap_out.at[slot],
                    swap_in.at[slot],
                    swap_send.at[slot],
                    swap_recv.at[slot],
                    partner,
                )
                accs[slot][:, :share] = value[:, :share]
            for slot, (left_side, factor) in enumerate(((powers, scale), (grads, slope))):
                value = (nn(left_side, kv[1 - slot]) * factor).astype(jnp.bfloat16)
                for step, index in enumerate(group):
                    block = value[step * rows : (step + 1) * rows]
                    if not index:
                        outs[slot][0, :, columns] = block
                        continue
                    stage[slot, index - 1] = block
                    remote(
                        stage.at[slot, index - 1],
                        outs[slot].at[0, :, columns],
                        row_send.at[slot, index - 1],
                        out_recv.at[slot, unit],
                        {"fine": order[index] * CORES + core},
                    )

        def give(slot, index, at):
            for to_sub, to_dp in plane + [(sub, dp)]:
                piece = (at * n_sub + to_sub) * n_dp + to_dp
                src = total_out.at[slot, pl.ds(pl.multiple_of(half + piece * mine, mine), mine)]
                dst = coarse_outs[slot].at[dp, :, head_columns(sub * heads + unit)]
                if index == 0 and to_sub is sub and to_dp is dp:
                    pltpu.make_async_copy(src, dst, coarse_recv.at[slot]).start()
                else:
                    remote(
                        src,
                        dst,
                        coarse_send.at[slot],
                        coarse_recv.at[slot],
                        (at * CORES + core, to_sub, to_dp),
                    )
            block = total_out.at[slot, block_of(at, rows)]
            result = outs[2 + slot]
            if index:
                remote(
                    block,
                    result.at[0, :, columns],
                    key_send.at[slot, index - 1],
                    out_recv.at[2 + slot, unit],
                    {"fine": at * CORES + core},
                )
            else:
                result[0, :, columns] = block[...]

        for slot in (1, 0):
            wait_bytes(swap_in.at[slot], swap_recv.at[slot])
            total_out[slot] = jnp.transpose(
                (accs[slot][:, :share] + swap_in[slot].astype(jnp.float32)).astype(jnp.bfloat16)
            )
            if chips > CORES:
                give(slot, 1, given[0])
        for index, at in list(enumerate(given))[1 if chips > CORES else 0 :]:
            for slot in (1, 0):
                give(slot, index + 1, at)
        for slot in (1, 0):
            give(slot, 0, chip)

    for head in range(heads):

        @pl.when(first_host + head != chip)
        def _(head=head):
            for slot, result in enumerate(outs):
                wait_bytes(
                    result.at[0, :, head * HEAD : (head + 1) * HEAD], out_recv.at[slot, head]
                )

    for slot, result in enumerate(coarse_outs):
        wait_bytes(result, coarse_recv.at[slot])
    for index in range(len(plane)):
        wait_bytes(c_src.at[:, 0, :, : heads * HEAD], plane_send.at[index])
    for head in range(heads):

        @pl.when(first_host + head != chip)
        def _(head=head):
            wait_bytes(kv_src.at[:, :, :HEAD], kv_send.at[head])
            wait_bytes(plane_in.at[:, :, :HEAD], c_send.at[head])
            wait_bytes(qg_src.at[:, :, :HEAD], qg_send.at[head])

    @pl.when(hosting)
    def _():
        for index in range(chips):
            wait_bytes(kv.at[:, :rows], near_send.at[index])
            wait_bytes(kv.at[:, half : half + crows], near_send.at[chips + index])
        for slot in range(2):
            wait_bytes(swap_out.at[slot], swap_send.at[slot])
            for index in range(chips - 1):
                wait_bytes(stage.at[slot, index], row_send.at[slot, index])
                wait_bytes(total_out.at[slot, :rows], key_send.at[slot, index])
            wait_bytes(total_out.at[slot, : chips * crows - mine], coarse_send.at[slot])


def fits_hosts(sizes, queries):
    chips, heads = sizes[0] // CORES, queries.shape[2] // HEAD
    return heads == CORES and chips % 2 == 0 and chips <= 2 * CORES


def hosted(sizes, queries, keys, values, out_grad, coarse_keys, coarse_values, fine_scale):
    n_fine, n_sub, n_dp = sizes
    rows, width = queries.shape[1:]
    heads, chips, mine = width // HEAD, n_fine // CORES, coarse_keys.shape[1]
    crows = mine * n_sub * n_dp
    share = chips * (rows + crows)
    total = CORES * share
    bf16, f32 = jnp.bfloat16, jnp.float32
    dma = pltpu.SemaphoreType.DMA
    return pl.pallas_call(
        functools.partial(host_kernel, sizes),
        out_shape=[jax.ShapeDtypeStruct(queries.shape, bf16)] * 4
        + [jax.ShapeDtypeStruct(coarse_keys.shape, bf16)] * 2,
        in_specs=[pl.BlockSpec(memory_space=pltpu.HBM)] * 7,
        out_specs=[pl.BlockSpec(memory_space=pltpu.VMEM)] * 6,
        scratch_shapes=[
            pltpu.VMEM((1, fine_scale.shape[0]), jnp.int32),
            pltpu.VMEM((2, rows, width), bf16),
            pltpu.VMEM((2, rows, width), bf16),
            pltpu.VMEM((2,) + coarse_keys.shape, bf16),
            pltpu.VMEM((2, crows, width), bf16),
            pltpu.VMEM((2, total, HEAD), bf16),
            pltpu.VMEM((2, HEAD, total), bf16),
            pltpu.VMEM((2, chips * rows, HEAD), bf16),
            pltpu.VMEM((2, chips - 1, rows, HEAD), bf16),
            pltpu.VMEM((HEAD, total), f32),
            pltpu.VMEM((HEAD, total), f32),
            pltpu.VMEM((2, HEAD, share), bf16),
            pltpu.VMEM((2, HEAD, share), bf16),
            pltpu.VMEM((2, share, HEAD), bf16),
            dma((9,)),
            dma((4,)),
            dma,
            dma((chips,)),
            dma((chips,)),
            dma((chips,)),
            dma((2 * chips,)),
            dma((2,)),
            dma((4, heads)),
            dma((2,)),
            dma((n_sub * n_dp - 1,)),
            dma((heads,)),
            dma((heads,)),
            dma((heads,)),
            dma((2 * chips,)),
            dma((2,)),
            dma((2, chips - 1)),
            dma((2, chips - 1)),
            dma((2,)),
        ],
        compiler_params=pltpu.CompilerParams(
            collective_id=0, has_side_effects=True, vmem_limit_bytes=48 * 1024 * 1024
        ),
    )(
        *(
            pltpu.with_memory_space_constraint(argument, pltpu.HBM)
            for argument in (
                queries,
                keys,
                values,
                out_grad,
                coarse_keys,
                coarse_values,
                fine_scale.reshape(1, fine_scale.shape[0]),
            )
        )
    )


def place(count, *refs):
    sem = refs[2 * count]
    stores = [
        pltpu.make_async_copy(refs[i], refs[count + i], sem.at[i]) for i in range(count)
    ]
    for store in stores:
        store.start()
    for store in stores:
        store.wait()


def placed_out(results):
    count = len(results)
    return pl.pallas_call(
        functools.partial(place, count),
        out_shape=[jax.ShapeDtypeStruct(result.shape, result.dtype) for result in results],
        in_specs=[pl.BlockSpec(memory_space=pltpu.VMEM)] * count,
        out_specs=[pl.BlockSpec(memory_space=pltpu.HBM)] * count,
        scratch_shapes=[pltpu.SemaphoreType.DMA((count,))],
        compiler_params=pltpu.CompilerParams(vmem_limit_bytes=8 * 1024 * 1024),
    )(*results)


def shards(sizes, queries, keys, values, out_grad, coarse_keys, coarse_values, fine_scale):
    direct = coarse_keys.shape[1] % 16 == 0
    fine = (queries, keys, values, out_grad)
    if direct:
        call = hosted if fits_hosts(sizes, queries) else functools.partial(fused, direct=True)
        return tuple(placed_out(call(sizes, *fine, coarse_keys, coarse_values, fine_scale)))

    def gathered(coarse):
        image = lax.all_to_all(coarse, "dp", split_axis=0, concat_axis=1, tiled=True)
        return lax.all_to_all(image, "sub", split_axis=2, concat_axis=1, tiled=True)

    def returned(grad):
        back = lax.all_to_all(grad, "sub", split_axis=1, concat_axis=2, tiled=True)
        return lax.all_to_all(back, "dp", split_axis=1, concat_axis=0, tiled=True)

    results = fused(
        sizes, *fine, gathered(coarse_keys), gathered(coarse_values), fine_scale, direct=False
    )
    return tuple(results[:4]) + (returned(results[4]), returned(results[5]))


def solution(mesh):
    sizes = tuple(mesh.shape[name] for name in ("fine", "sub", "dp"))
    placed = P("dp", "fine", "sub")
    coarse = P(None, ("fine", "sub", "dp"), None)
    return jax.shard_map(
        functools.partial(shards, sizes),
        mesh=mesh,
        in_specs=(placed,) * 4 + (coarse, coarse, P()),
        out_specs=(placed,) * 4 + (coarse, coarse),
        check_vma=False,
    )
```
